32 devices in a mesh: gx: 16 (over z, y, x), gy: 2 (over core).
Axes of the slice: x: 2, y: 2, z: 4, core: 2. Of those that a mesh axis runs over, the one named last changes fastest.
Arguments:
- sources: bfloat16 [2048, 8, 128], P(('gx', 'gy')), may hold values from -6 to 6
- owners: int32 [2048, 1], P(('gx', 'gy')), may hold values from 0 to 15; in each aligned block of 64 rows (0 to 63, 64 to 127, ...) at most 8 rows name the same one
- strip_rows: int32 [2048], P(('gx', 'gy')), may hold values from 0 to 255
- panel_counts: int32 [2048], P(('gx', 'gy')), may hold values from 1 to 128
- arrival_bins: int32 [4096, 4, 128], P('gx'), may hold values from 0 to 254
- arrival_fracs: float32 [4096, 4, 128], P('gx'), may hold values from 0 to 1
- gain_table: bfloat16 [4096, 8, 4, 1024], P('gx'), may hold values from -0.125 to 0.125
Outputs:
- signals: float32 [1024, 4, 256], P(('gx', 'gy'))
The draws below stay inside these ranges and needn't reach their ends.
Inputs may be any that keep to these rules, and one draw needn't show every extreme that they name: `owners`: among the rows of one device, at most 8 strips name one patch, a bound that some block reaches.
All inputs are finite; a program needn't handle non-finite values.
Results may differ from the reference program's by a relative error of at most 0.0044.
Values may be sent and summed in bfloat16 or wider, within the bound.
No kernel may reach another device: no remote copies, remote signals or barrier semaphores. Data moves between devices by JAX's collectives and lax.ppermute only.
A program may use at most 768 MiB of HBM per device.

```python
import math
import jax
import jax.numpy as jnp
import numpy as np
from jax import lax

TERMS = 8
SP = 128
NBIN = 256
NOB = 4
OBS_BLOCK = 1024
STRIP_DEV = 64
ROWS = 256
CAP = 8
STRIPS = 2048
TROWS = 4096
N_GX = 16


def set_ends(array, stream_key, low, high):
    longest = array.shape.index(max(array.shape))
    spots = []
    for shift in (0, 1):
        where = [jax.random.randint(jax.random.fold_in(stream_key, axis), (), 0, length) for axis, length in enumerate(array.shape)]
        where[longest] = (where[longest] + shift) % array.shape[longest]
        spots.append(tuple(where))
    return array.at[spots[0]].set(low).at[spots[1]].set(high)


def spiked(drawn, key, source, target, shards_of, factor):
    owner, partner = [(jnp.arange(drawn.shape[axis_at]) // (drawn.shape[axis_at] // shards_of)).reshape([-1 if axis == axis_at else 1 for axis in range(drawn.ndim)]) for axis_at in (source, target)]
    chosen = jax.random.permutation(key, shards_of)[partner]
    strong = (owner == chosen) | (owner == (partner + shards_of // 2) % shards_of)
    return jnp.where(strong, factor * drawn, drawn)


def level_of(own_key, shape, pieces, low, largest):
    def one(position, parts):
        heights = jax.random.uniform(jax.random.fold_in(jax.random.fold_in(own_key, 6), position), (parts,), jnp.float32, low / len(pieces), largest / len(pieces))
        return jnp.repeat(jnp.exp(heights), shape[position] // parts).reshape((-1,) + (1,) * (len(shape) - position - 1))

    level = one(*pieces[0])
    for cut in pieces[1:]:
        level = level * one(*cut)
    return level


def assign_block(key, own, number, rows, count, top, most, slope):
    order = jax.random.permutation(key, count)
    crowded, usual = portions_of(count, rows * top, most, slope, True), portions_of(count, rows * top, most, slope, False)
    places = jnp.arange(count)

    def named(sizes, turn):
        used = int((sizes > 0).sum())
        fixed = max(1, used // 4)
        passed = fixed + (places - fixed + turn * (used - fixed)) % max(1, count - fixed)
        return jnp.zeros((count,), jnp.int32).at[order[jnp.where(places < fixed, places, passed)]].set(jnp.asarray(sizes, jnp.int32))

    sizes = jnp.where(number % 4 == 0, named(crowded, number // 4), named(usual, number - number // 4 - 1))
    mixed = jax.random.permutation(jax.random.fold_in(own, 3), count)
    donor, receiver = mixed[0:count // 2 * 2:2], mixed[1:count // 2 * 2:2]
    slack = jnp.minimum(sizes[donor] - 1, most - sizes[receiver]) // 2
    slack = jnp.where((donor == order[0]) | (receiver == order[0]) | (sizes[receiver] == 0), 0, jnp.maximum(slack, 0))
    passed = jax.random.randint(jax.random.fold_in(own, 4), (count // 2,), 0, 1 << 20) % (slack + 1)
    sizes = sizes.at[donor].add(-passed).at[receiver].add(passed)
    members = jnp.searchsorted(jnp.cumsum(sizes), jnp.arange(rows * top), side="right").astype(jnp.int32)
    listing = members.reshape(top, rows).T
    listing = listing[jax.random.permutation(jax.random.fold_in(own, 1), rows)]
    turn = jax.random.randint(jax.random.fold_in(own, 2), (rows, 1), 0, top)
    return jnp.take_along_axis(listing, (jnp.arange(top)[None, :] + turn) % top, axis=1)


def portions_of(count, total, reach, slope, full):
    loads = [(1 << 20) // math.isqrt(standing ** slope) + 1 for standing in range(1, count + 1)]
    largest = reach if full else min(reach, max(-(-total // count), total * loads[0] // sum(loads)))
    least = 1 if total - largest >= count - 1 else 0
    holding, surplus = [largest] + [least] * (count - 1), total - largest - least * (count - 1)
    while surplus > 0:
        free = [i for i in range(1, count) if holding[i] < largest] or [i for i in range(1, count) if holding[i] < reach]
        pool, budget = sum([loads[i] for i in free]), surplus
        for i in free:
            more = min(reach - holding[i], max(1, budget * loads[i] // pool), surplus)
            holding[i] = holding[i] + more
            surplus = surplus - more
    return np.array(holding)


def gaussian(rng, dims, spread, most, shards=(), held_as=jnp.bfloat16):
    values = spread * jax.random.normal(rng, dims, jnp.float32)
    if shards:
        values = values * level_of(rng, dims, shards, -0.22, 0.18)
    return jnp.clip(values, -most, most).astype(held_as)


def bell_draw_with(key, shape, width, limit, split, heavy, kind=jnp.bfloat16):
    result = width * jax.random.normal(key, shape, jnp.float32)
    if split:
        result = result * level_of(key, shape, split, -0.22, 0.18)
    return jnp.clip(spiked(result, jax.random.fold_in(key, 3), *heavy), -limit, limit).astype(kind)


def setup_inputs(seed: int = 0) -> dict:
    arg_keys = jax.random.split(jax.random.key(seed), 8)
    sources = gaussian(arg_keys[0], (STRIPS, TERMS, SP), 1.0, 6.0, ((0, 32),))
    owners_keys = jax.random.split(jax.random.fold_in(arg_keys[1], 1), STRIPS // STRIP_DEV)
    owners_turns = jax.random.permutation(jax.random.fold_in(arg_keys[1], 3), STRIPS // STRIP_DEV)
    owners = jax.vmap(lambda own, number: assign_block(jax.random.fold_in(arg_keys[1], 2), own, number, STRIP_DEV, N_GX, 1, CAP, 2))(owners_keys, owners_turns).reshape((STRIPS, 1))
    strip_rows = set_ends(jax.random.randint(arg_keys[2], (STRIPS,), 0, ROWS), jax.random.fold_in(arg_keys[2], 1), 0, ROWS - 1).astype(jnp.int32)
    panel_counts = set_ends(jax.random.randint(arg_keys[3], (STRIPS,), 1, SP + 1), jax.random.fold_in(arg_keys[3], 1), 1, SP).astype(jnp.int32)
    arrival_bins = set_ends(jax.random.randint(arg_keys[4], (TROWS, NOB, SP), 0, NBIN - 1), jax.random.fold_in(arg_keys[4], 1), 0, (NBIN - 1) - 1).astype(jnp.int32)
    arrival_fracs = jnp.clip(1.0 * jax.random.uniform(arg_keys[5], (TROWS, NOB, SP), jnp.float32) ** level_of(arg_keys[5], (TROWS, NOB, SP), ((0, 16),), -0.2, 0.2), 0.0, 1.0)
    gain_table = bell_draw_with(arg_keys[6], (TROWS, TERMS, NOB, OBS_BLOCK), TROWS ** -0.5, 0.125, ((0, 16),), (0, 3, 16, 2.0))
    return {"sources": sources, "owners": owners, "strip_rows": strip_rows, "panel_counts": panel_counts, "arrival_bins": arrival_bins, "arrival_fracs": arrival_fracs, "gain_table": gain_table}


def interp_weights(bin_ids, fractions):
    positions = jnp.arange(NBIN, dtype=jnp.int32)
    lower = jnp.where(positions[None, None, :] == bin_ids[:, :, None], 1.0 - fractions[:, :, None], 0.0)
    upper = jnp.where(positions[None, None, :] == bin_ids[:, :, None] + 1, fractions[:, :, None], 0.0)
    return (lower + upper).astype(jnp.bfloat16)


def reference(sources, owners, strip_rows, panel_counts, arrival_bins, arrival_fracs, gain_table):
    live_mask = (jnp.arange(SP, dtype=jnp.int32)[None, :] < panel_counts[:, None]).astype(jnp.float32)
    masked = sources.astype(jnp.float32) * live_mask[:, None, :]
    global_rows = (owners[:, 0] * ROWS + strip_rows).astype(jnp.int32)
    row_sources = jax.ops.segment_sum(masked, global_rows, num_segments=ROWS * N_GX)
    row_rounded = row_sources.astype(jnp.bfloat16)

    def patch_term(running, patch_index):
        first_row = (patch_index * ROWS).astype(jnp.int32)
        patch_sources = lax.dynamic_slice_in_dim(row_rounded, first_row, ROWS, 0).astype(jnp.float32)
        patch_bins = lax.dynamic_slice_in_dim(arrival_bins, first_row, ROWS, 0)
        patch_fracs = lax.dynamic_slice_in_dim(arrival_fracs, first_row, ROWS, 0)
        patch_gains = lax.dynamic_slice_in_dim(gain_table, first_row, ROWS, 0).astype(jnp.float32)
        for block_index in range(NOB):
            weights = interp_weights(patch_bins[:, block_index, :], patch_fracs[:, block_index, :]).astype(jnp.float32)
            arrived = jnp.einsum('rkp,rpb->rkb', patch_sources, weights, precision=lax.Precision.HIGHEST)
            arrived_rounded = arrived.astype(jnp.bfloat16).astype(jnp.float32)
            added = jnp.einsum('rkt,rkb->tb', patch_gains[:, :, block_index, :], arrived_rounded, precision=lax.Precision.HIGHEST)
            running = running.at[:, block_index, :].add(added)
        return running, None

    start_value = jnp.zeros((OBS_BLOCK, NOB, NBIN), jnp.float32)
    signals, unused = lax.scan(patch_term, start_value, jnp.arange(N_GX, dtype=jnp.int32))
    return signals
```

```python
import functools

import jax
import jax.numpy as jnp
from jax import lax
from jax.experimental import pallas as pl
from jax.experimental.pallas import tpu as pltpu
from jax.sharding import PartitionSpec as P

NBIN = 256
LANES = 128
STEP = 512
F32 = jnp.float32
BF16 = jnp.bfloat16
VMEM = pl.BlockSpec(memory_space=pltpu.VMEM)


def iota(shape, axis):
    return lax.broadcasted_iota(jnp.int32, shape, axis)


def pack_kernel(slots, src_ref, own_ref, row_ref, cnt_ref, out_ref, held):
    strips, terms, panels = src_ref.shape
    shards = out_ref.shape[0]
    own_row = own_ref[...].astype(F32)
    same = iota((strips, strips), 0) == iota((strips, strips), 1)
    earlier = iota((strips, strips), 0) < iota((strips, strips), 1)
    own_col = jnp.sum(jnp.where(same, own_row, 0.0), axis=1, keepdims=True)
    cnt_col = jnp.sum(jnp.where(same, cnt_ref[...].astype(F32), 0.0), axis=1, keepdims=True)
    ranks = jnp.sum(
        jnp.where(jnp.logical_and(own_col == own_row, earlier), 1.0, 0.0), axis=0, keepdims=True
    )
    slot_row = own_row * slots + ranks
    total = shards * slots
    placed = iota((total, strips), 0).astype(F32) == slot_row
    placing = jnp.where(placed, 1.0, 0.0).astype(BF16)
    rows = (
        jnp.sum(jnp.where(placed, row_ref[...].astype(F32) + 1.0, 0.0), axis=1, keepdims=True) - 1.0
    )
    held[...] = src_ref[...].astype(F32).reshape(strips * terms, panels)
    live = iota((strips, panels), 1).astype(F32) < cnt_col
    for first in range(0, terms, 2):
        pair = []
        for term in (first, first + 1):
            masked = jnp.where(live, held[pl.ds(term, strips, stride=terms), :], 0.0).astype(BF16)
            moved = jnp.dot(placing, masked, preferred_element_type=F32)
            pair.append(moved.reshape(shards, slots, panels))
        out_ref[:, first * slots : (first + 2) * slots, :] = jnp.concatenate(pair, axis=1).astype(
            BF16
        )
    out_ref[:, terms * slots :, :] = (
        jnp.broadcast_to(rows, (total, panels)).reshape(shards, slots, panels).astype(BF16)
    )


PAIRS = 32


def gains_kernel(blocks, first_ref, view_ref, out_ref, held):
    count, pitch, lanes = held.shape
    group = view_ref.shape[0] // count
    held[:, :group, :] = view_ref[...].astype(F32).reshape(count, group, lanes)
    flat = held.reshape(count * pitch, lanes)
    for part in range(group // blocks):
        for turn in range(out_ref.shape[0]):
            taken = flat[pl.ds(first_ref[0] + turn + part * blocks, count, stride=pitch), :]
            out_ref[turn, :, part * lanes : (part + 1) * lanes] = taken.astype(BF16)


def signal_kernel(slots, terms, columns, *refs):
    got_refs, (bin_ref, frac_ref, gain_ref, out_ref) = refs[:columns], refs[columns : columns + 4]
    held, src, arr, gains, low, high, at, sem = refs[columns + 4 :]
    own, row_count, panels = bin_ref.shape
    devices, _, share, _ = out_ref.shape
    copies = [
        pltpu.make_async_copy(gain_ref.at[turn], gains.at[turn], sem.at[turn])
        for turn in range(own)
    ]
    for copy in copies:
        copy.start()
    low[...] = 1.0 - frac_ref[...]
    high[...] = frac_ref[...]
    at[...] = bin_ref[...].astype(F32)

    def taken(term):
        parts = [
            ref[:, term * slots : (term + 1) * slots, :].astype(F32).reshape(-1, panels)
            for ref in got_refs
        ]
        return jnp.concatenate(parts, axis=0)

    rows = taken(terms)
    hot_t = jnp.concatenate(
        [
            jnp.where(rows == (iota(rows.shape, 1) + start).astype(F32), 1.0, 0.0)
            for start in range(0, row_count, panels)
        ],
        axis=1,
    )
    hot = hot_t.T.astype(BF16)
    for term in range(terms):
        held[pl.ds(term, row_count, stride=terms), :] = jnp.dot(
            hot, taken(term).astype(BF16), preferred_element_type=F32
        )
    src[...] = held[...].astype(BF16)

    half = 2 * terms
    upper = iota((half, panels), 0) < terms
    place = iota((half, panels), 0).astype(F32)

    def spread(value):
        return jnp.broadcast_to(value, (half, panels))

    def weights(turn, row):
        here = at[turn, pl.ds(row, 1), :]
        tile = jnp.floor(here * (1.0 / half))
        inner = spread(here - half * tile)
        tile = spread(tile).astype(BF16)
        low_w, high_w = spread(low[turn, pl.ds(row, 1), :]), spread(high[turn, pl.ds(row, 1), :])
        body = jnp.where(
            place == inner, low_w, jnp.where(place == inner + 1.0, high_w, 0.0)
        ).astype(BF16)
        spill = jnp.where(place + float(half - 1) == inner, high_w, 0.0).astype(BF16)
        zero = jnp.zeros((half, panels), BF16)
        tiles, before = [], None
        for index in range(NBIN // half):
            match = tile == jnp.full((half, panels), index, BF16)
            rest = zero if before is None else jnp.where(before, spill, zero)
            tiles.append(jnp.where(match, body, rest))
            before = match
        return jnp.concatenate(tiles, axis=0)

    for turn in range(own):

        def step(index, carry, turn=turn):
            for inner in range(PAIRS):
                pair = index * PAIRS + inner
                where = pl.ds(pl.multiple_of(pair * half, half), half)
                rows16 = src[where, :]
                zero = jnp.zeros_like(rows16)
                lhs = jnp.concatenate(
                    [jnp.where(upper, rows16, zero), jnp.where(upper, zero, rows16)], axis=1
                )
                rhs = jnp.concatenate(
                    [weights(turn, 2 * pair), weights(turn, 2 * pair + 1)], axis=1
                )
                binned = lax.dot_general(
                    lhs, rhs, (((1,), (1,)), ((), ())), preferred_element_type=F32
                )
                arr[where, :] = binned.astype(BF16)
            return carry

        lax.fori_loop(0, row_count // (2 * PAIRS), step, 0)
        copies[turn].wait()
        out_t = lax.dot_general(
            arr[...], gains[turn], (((0,), (0,)), ((), ())), preferred_element_type=F32
        )
        out_ref[:, turn] = out_t.T.astype(BF16).reshape(devices, share, NBIN)


def on_device(sources, owners, strip_rows, panel_counts, arrival_bins, arrival_fracs, gain_table):
    strips, terms, panels = sources.shape
    shards = lax.axis_size("gx")
    columns = lax.axis_size("gy")
    cap = 2 * strips // shards
    slots = -(-cap // 8) * 8
    rows_here, blocks = arrival_bins.shape[:2]
    observers = gain_table.shape[3]
    own = blocks // columns
    devices = shards * columns
    assert rows_here <= 256 and blocks % columns == 0

    send = pl.pallas_call(
        functools.partial(pack_kernel, slots),
        out_shape=jax.ShapeDtypeStruct((shards, (terms + 1) * slots, panels), BF16),
        in_specs=[VMEM] * 4,
        out_specs=VMEM,
        scratch_shapes=[pltpu.VMEM((strips * terms, panels), F32)],
        name="pack",
    )(sources, owners.reshape(1, strips), strip_rows.reshape(1, strips), panel_counts.reshape(1, strips))

    got = lax.all_to_all(send, "gx", split_axis=0, concat_axis=0, tiled=True)
    first = lax.axis_index("gy") * own
    group = blocks * (observers // LANES)
    view = (
        gain_table.reshape(rows_here * terms, blocks, observers // LANES, LANES)
        .transpose(0, 2, 1, 3)
        .reshape(rows_here * terms * group, LANES)
    )
    own_gains = pl.pallas_call(
        functools.partial(gains_kernel, blocks),
        out_shape=jax.ShapeDtypeStruct((own, rows_here * terms, observers), BF16),
        grid_spec=pltpu.PrefetchScalarGridSpec(
            num_scalar_prefetch=1,
            grid=(rows_here * terms // STEP,),
            in_specs=[pl.BlockSpec((STEP * group, LANES), lambda i, f: (i, 0))],
            out_specs=pl.BlockSpec((own, STEP, observers), lambda i, f: (0, i, 0)),
            scratch_shapes=[pltpu.VMEM((STEP, group + 8, LANES), F32)],
        ),
        name="gains",
        cost_estimate=pl.CostEstimate(
            flops=20 * gain_table.size, bytes_accessed=3 * gain_table.size, transcendentals=0
        ),
    )(first.reshape(1), view)
    bins = jnp.transpose(lax.dynamic_slice_in_dim(arrival_bins, first, own, 1), (1, 0, 2))
    fracs = jnp.transpose(lax.dynamic_slice_in_dim(arrival_fracs, first, own, 1), (1, 0, 2))
    got, own_gains, bins, fracs = lax.optimization_barrier((got, own_gains, bins, fracs))
    parts = [got]
    for turn in range(1, columns):
        parts.append(
            lax.ppermute(got, "gy", [(i, (i + turn) % columns) for i in range(columns)])
        )
    share = observers // devices
    partial = pl.pallas_call(
        functools.partial(signal_kernel, slots, terms, columns),
        out_shape=jax.ShapeDtypeStruct((devices, own, share, NBIN), BF16),
        in_specs=[VMEM] * (columns + 2) + [pl.BlockSpec(memory_space=pltpu.HBM)],
        out_specs=VMEM,
        scratch_shapes=[
            pltpu.VMEM((rows_here * terms, panels), F32),
            pltpu.VMEM((rows_here * terms, panels), BF16),
            pltpu.VMEM((rows_here * terms, NBIN), BF16),
            pltpu.VMEM((own, rows_here * terms, observers), BF16),
            pltpu.VMEM((own, rows_here, panels), F32),
            pltpu.VMEM((own, rows_here, panels), F32),
            pltpu.VMEM((own, rows_here, panels), F32),
            pltpu.SemaphoreType.DMA((own,)),
        ],
        name="signal",
        compiler_params=pltpu.CompilerParams(vmem_limit_bytes=48 << 20),
        cost_estimate=pl.CostEstimate(
            flops=2 * own * rows_here * terms * NBIN * (observers + panels * 8),
            bytes_accessed=2 * own * rows_here * terms * observers,
            transcendentals=0,
        ),
    )(*parts, bins, fracs, own_gains)
    got = lax.all_to_all(partial, ("gx", "gy"), split_axis=0, concat_axis=0, tiled=True)
    sums = jnp.sum(got.reshape(shards, columns, own, share, NBIN).astype(F32), axis=0)
    return jnp.transpose(sums.reshape(blocks, share, NBIN), (1, 0, 2))


def solution(mesh):
    placed = (
        P(("gx", "gy"), None, None),
        P(("gx", "gy"), None),
        P(("gx", "gy")),
        P(("gx", "gy")),
        P("gx", None, None),
        P("gx", None, None),
        P("gx", None, None, None),
    )
    return jax.shard_map(
        on_device,
        mesh=mesh,
        in_specs=placed,
        out_specs=P(("gx", "gy"), None, None),
        check_vma=False,
    )
```

```python
import functools

import jax
import jax.numpy as jnp
from jax import lax
from jax.experimental import pallas as pl
from jax.experimental.pallas import tpu as pltpu
from jax.sharding import PartitionSpec as P

NBIN = 256
LANES = 128
STEP = 128
DEPTH = 8
SPARE = 4
F32 = jnp.float32
BF16 = jnp.bfloat16
VMEM = pl.BlockSpec(memory_space=pltpu.VMEM)
SMEM = pl.BlockSpec(memory_space=pltpu.SMEM)
HBM = pl.BlockSpec(memory_space=pltpu.HBM)


def iota(shape, axis):
    return lax.broadcasted_iota(jnp.int32, shape, axis)


def pack_kernel(slots, src_ref, own_ref, row_ref, cnt_ref, out_ref, held):
    strips, terms, panels = src_ref.shape
    shards = out_ref.shape[0]
    own_row = own_ref[...].astype(F32)
    same = iota((strips, strips), 0) == iota((strips, strips), 1)
    earlier = iota((strips, strips), 0) < iota((strips, strips), 1)
    own_col = jnp.sum(jnp.where(same, own_row, 0.0), axis=1, keepdims=True)
    cnt_col = jnp.sum(jnp.where(same, cnt_ref[...].astype(F32), 0.0), axis=1, keepdims=True)
    ranks = jnp.sum(
        jnp.where(jnp.logical_and(own_col == own_row, earlier), 1.0, 0.0), axis=0, keepdims=True
    )
    slot_row = own_row * slots + ranks
    total = shards * slots
    placed = iota((total, strips), 0).astype(F32) == slot_row
    placing = jnp.where(placed, 1.0, 0.0).astype(BF16)
    rows = (
        jnp.sum(jnp.where(placed, row_ref[...].astype(F32) + 1.0, 0.0), axis=1, keepdims=True) - 1.0
    )
    held[...] = src_ref[...].astype(F32).reshape(strips * terms, panels)
    live = iota((strips, panels), 1).astype(F32) < cnt_col
    for first in range(0, terms, 2):
        pair = []
        for term in (first, first + 1):
            masked = jnp.where(live, held[pl.ds(term, strips, stride=terms), :], 0.0).astype(BF16)
            moved = jnp.dot(placing, masked, preferred_element_type=F32)
            pair.append(moved.reshape(shards, slots, panels))
        out_ref[:, first * slots : (first + 2) * slots, :] = jnp.concatenate(pair, axis=1).astype(
            BF16
        )
    out_ref[:, terms * slots :, :] = (
        jnp.broadcast_to(rows, (total, panels)).reshape(shards, slots, panels).astype(BF16)
    )


PAIRS = 64


def gains_kernel(blocks, first_ref, view_ref, out_ref, inward, outward, in_sem, out_sem):
    depth, taken_rows, lanes = inward.shape
    spare, own, count, observers = outward.shape
    tiles = observers // lanes
    group = taken_rows // count
    steps = view_ref.shape[0] // taken_rows
    chunk = 8 * group
    shape = (own * tiles * 8, chunk)
    to, come = iota(shape, 0), iota(shape, 1)
    block = first_ref[0] + to // (8 * tiles)
    wanted = (to % 8) * group + (to // 8 % tiles) * blocks + block
    pick = jnp.where(come == wanted, 1.0, 0.0).astype(BF16)

    def fetch(step):
        slot = lax.rem(step, depth)
        return pltpu.make_async_copy(
            view_ref.at[pl.ds(pl.multiple_of(step * taken_rows, taken_rows), taken_rows), :],
            inward.at[slot],
            in_sem.at[slot],
        )

    def leave(step):
        slot = lax.rem(step, spare)
        return pltpu.make_async_copy(
            outward.at[slot],
            out_ref.at[:, pl.ds(pl.multiple_of(step * count, count), count), :],
            out_sem.at[slot],
        )

    for step in range(depth - 1):
        fetch(step).start()

    def body(step, carry):
        @pl.when(step + depth - 1 < steps)
        def _():
            fetch(step + depth - 1).start()

        fetch(step).wait()

        @pl.when(step >= spare)
        def _():
            leave(step - spare).wait()

        slot, held = lax.rem(step, spare), lax.rem(step, depth)
        for at in range(0, count, 16):
            pair = jnp.concatenate(
                [
                    inward[held, at * group : at * group + chunk, :],
                    inward[held, at * group + chunk : at * group + 2 * chunk, :],
                ],
                axis=1,
            )
            taken = jnp.dot(pick, pair, preferred_element_type=F32)
            for turn in range(own):
                for tile in range(tiles):
                    start = (turn * tiles + tile) * 8
                    both = jnp.concatenate(
                        [taken[start : start + 8, :lanes], taken[start : start + 8, lanes:]], axis=0
                    )
                    outward[slot, turn, at : at + 16, tile * lanes : (tile + 1) * lanes] = (
                        both.astype(BF16)
                    )
        leave(step).start()
        return carry

    lax.fori_loop(0, steps, body, 0)
    for step in range(steps - spare, steps):
        leave(step).wait()


def sum_rows(slots, terms, got_refs, held, src):
    panels = src.shape[1]
    row_count = src.shape[0] // terms

    def taken(term):
        parts = [
            ref[:, term * slots : (term + 1) * slots, :].astype(F32).reshape(-1, panels)
            for ref in got_refs
        ]
        return jnp.concatenate(parts, axis=0)

    rows = taken(terms)
    hot_t = jnp.concatenate(
        [
            jnp.where(rows == (iota(rows.shape, 1) + start).astype(F32), 1.0, 0.0)
            for start in range(0, row_count, panels)
        ],
        axis=1,
    )
    hot = hot_t.T.astype(BF16)
    for term in range(terms):
        held[pl.ds(term, row_count, stride=terms), :] = jnp.dot(
            hot, taken(term).astype(BF16), preferred_element_type=F32
        )
    src[...] = held[...].astype(BF16)


def signal_kernel(slots, terms, columns, lines, turn, *refs):
    opening = turn == 0
    if opening:
        got_refs, refs = refs[:columns], refs[columns:]
        block_ref, bin_ref, frac_ref, gain_ref, out_ref, src, held, arr, gains, turned, sem = refs
    else:
        block_ref, src, bin_ref, frac_ref, gain_ref, out_ref, arr, gains, turned, sem = refs
    row_count, _, panels = bin_ref.shape
    targets = out_ref.shape[0]
    copy = pltpu.make_async_copy(gain_ref.at[turn], gains, sem)
    copy.start()
    if opening:
        sum_rows(slots, terms, got_refs, held, src)
    block = block_ref[0] + turn
    half = 2 * terms
    upper = iota((half, panels), 0) < terms
    place = iota((half, panels), 0).astype(F32)

    def spread(value):
        return jnp.broadcast_to(value, (half, panels))

    def weights(row):
        here = bin_ref[row, pl.ds(block, 1), :].astype(F32)
        past = frac_ref[row, pl.ds(block, 1), :]
        tile = jnp.floor(here * (1.0 / half))
        inner = spread(here - half * tile)
        tile = spread(tile).astype(BF16)
        low_w, high_w = spread(1.0 - past), spread(past)
        body = jnp.where(
            place == inner, low_w, jnp.where(place == inner + 1.0, high_w, 0.0)
        ).astype(BF16)
        spill = jnp.where(place + float(half - 1) == inner, high_w, 0.0).astype(BF16)
        zero = jnp.zeros((half, panels), BF16)
        tiles, before = [], None
        for index in range(NBIN // half):
            match = tile == jnp.full((half, panels), index, BF16)
            rest = zero if before is None else jnp.where(before, spill, zero)
            tiles.append(jnp.where(match, body, rest))
            before = match
        return jnp.concatenate(tiles, axis=0)

    def step(index, carry):
        for inner in range(PAIRS):
            pair = index * PAIRS + inner
            where = pl.ds(pl.multiple_of(pair * half, half), half)
            rows16 = src[where, :]
            zero = jnp.zeros_like(rows16)
            lhs = jnp.concatenate(
                [jnp.where(upper, rows16, zero), jnp.where(upper, zero, rows16)], axis=1
            )
            rhs = jnp.concatenate([weights(2 * pair), weights(2 * pair + 1)], axis=1)
            if inner % 3 < 2:
                turned[inner] = rhs.T
                binned = jnp.dot(lhs, turned[inner], preferred_element_type=F32)
            else:
                binned = lax.dot_general(
                    lhs, rhs, (((1,), (1,)), ((), ())), preferred_element_type=F32
                )
            arr[where, :] = binned.astype(BF16)
        return carry

    lax.fori_loop(0, row_count // (2 * PAIRS), step, 0)
    copy.wait()
    out_t = lax.dot_general(
        arr[...], gains[...], (((0,), (0,)), ((), ())), preferred_element_type=F32
    )
    out = out_t.T.astype(BF16)
    piece = out.shape[0] // (targets * lines)
    for line in range(lines):
        for target in range(targets):
            start = (line * targets + target) * piece
            out_ref[target, line * piece : (line + 1) * piece, :] = out[start : start + piece, :]


def on_device(sources, owners, strip_rows, panel_counts, arrival_bins, arrival_fracs, gain_table):
    strips, terms, panels = sources.shape
    shards = lax.axis_size("gx")
    columns = lax.axis_size("gy")
    cap = 2 * strips // shards
    slots = -(-cap // 8) * 8
    rows_here, blocks = arrival_bins.shape[:2]
    observers = gain_table.shape[3]
    own = blocks // columns
    devices = shards * columns
    assert rows_here <= 256 and blocks % columns == 0

    send = pl.pallas_call(
        functools.partial(pack_kernel, slots),
        out_shape=jax.ShapeDtypeStruct((shards, (terms + 1) * slots, panels), BF16),
        in_specs=[VMEM] * 4,
        out_specs=VMEM,
        scratch_shapes=[pltpu.VMEM((strips * terms, panels), F32)],
        name="pack",
    )(sources, owners.reshape(1, strips), strip_rows.reshape(1, strips), panel_counts.reshape(1, strips))

    got = lax.all_to_all(send, "gx", split_axis=0, concat_axis=0, tiled=True)
    first = lax.axis_index("gy") * own
    group = blocks * (observers // LANES)
    view = (
        gain_table.reshape(rows_here * terms, blocks, observers // LANES, LANES)
        .transpose(0, 2, 1, 3)
        .reshape(rows_here * terms * group, LANES)
    )
    own_gains = pl.pallas_call(
        functools.partial(gains_kernel, blocks),
        out_shape=jax.ShapeDtypeStruct((own, rows_here * terms, observers), BF16),
        in_specs=[SMEM, HBM],
        out_specs=HBM,
        scratch_shapes=[
            pltpu.VMEM((DEPTH, STEP * group, LANES), BF16),
            pltpu.VMEM((SPARE, own, STEP, observers), BF16),
            pltpu.SemaphoreType.DMA((DEPTH,)),
            pltpu.SemaphoreType.DMA((SPARE,)),
        ],
        name="gains",
        cost_estimate=pl.CostEstimate(
            flops=20 * gain_table.size, bytes_accessed=3 * gain_table.size, transcendentals=0
        ),
    )(first.reshape(1), view)
    got, own_gains = lax.optimization_barrier((got, own_gains))
    parts = [got]
    for turn in range(1, columns):
        parts.append(
            lax.ppermute(got, "gy", [(i, (i + turn) % columns) for i in range(columns)])
        )
    share = observers // devices
    planes = 1
    while planes * planes < shards:
        planes *= 2
    lines = shards // planes
    in_plane = [[line * planes + i for i in range(planes)] for line in range(lines)]
    in_line = [
        [(line * planes + i) * columns + j for line in range(lines) for j in range(columns)]
        for i in range(planes)
    ]
    plane_sums, row_sources = [], None
    for turn in range(own):
        opening = turn == 0
        partial = jax.ShapeDtypeStruct((planes, lines * columns * share, NBIN), BF16)
        source = jax.ShapeDtypeStruct((rows_here * terms, panels), BF16)
        made = pl.pallas_call(
            functools.partial(signal_kernel, slots, terms, columns, lines, turn),
            out_shape=(partial, source) if opening else (partial,),
            in_specs=([VMEM] * columns + [SMEM] if opening else [SMEM, VMEM]) + [VMEM] * 2 + [HBM],
            out_specs=(VMEM, VMEM) if opening else (VMEM,),
            scratch_shapes=([pltpu.VMEM((rows_here * terms, panels), F32)] if opening else [])
            + [
                pltpu.VMEM((rows_here * terms, NBIN), BF16),
                pltpu.VMEM((rows_here * terms, observers), BF16),
                pltpu.VMEM((PAIRS, 2 * panels, NBIN), BF16),
                pltpu.SemaphoreType.DMA,
            ],
            name="signal",
            compiler_params=pltpu.CompilerParams(vmem_limit_bytes=48 << 20),
            cost_estimate=pl.CostEstimate(
                flops=2 * rows_here * terms * NBIN * (observers + panels * 8),
                bytes_accessed=2 * rows_here * terms * observers,
                transcendentals=0,
            ),
        )(
            *(parts + [first.reshape(1)] if opening else [first.reshape(1), row_sources]),
            arrival_bins,
            arrival_fracs,
            own_gains,
        )
        if opening:
            row_sources = made[1]
        met = lax.all_to_all(
            made[0], "gx", split_axis=0, concat_axis=0, axis_index_groups=in_plane, tiled=True
        )
        plane_sums.append(
            jnp.sum(met.astype(F32), axis=0).astype(BF16).reshape(lines * columns, share, NBIN)
        )
    met = lax.all_to_all(
        jnp.stack(plane_sums, axis=1),
        ("gx", "gy"),
        split_axis=0,
        concat_axis=0,
        axis_index_groups=in_line,
        tiled=True,
    )
    sums = jnp.sum(met.reshape(lines, columns, own, share, NBIN).astype(F32), axis=0)
    return jnp.transpose(sums.reshape(blocks, share, NBIN), (1, 0, 2))


def solution(mesh):
    placed = (
        P(("gx", "gy"), None, None),
        P(("gx", "gy"), None),
        P(("gx", "gy")),
        P(("gx", "gy")),
        P("gx", None, None),
        P("gx", None, None),
        P("gx", None, None, None),
    )
    return jax.shard_map(
        on_device,
        mesh=mesh,
        in_specs=placed,
        out_specs=P(("gx", "gy"), None, None),
        check_vma=False,
    )
```

```python
import functools

import jax
import jax.numpy as jnp
from jax import lax
from jax.experimental import pallas as pl
from jax.experimental.pallas import tpu as pltpu
from jax.sharding import PartitionSpec as P

NBIN = 256
LANES = 128
STEP = 128
DEPTH = 8
SPARE = 4
F32 = jnp.float32
BF16 = jnp.bfloat16
VMEM = pl.BlockSpec(memory_space=pltpu.VMEM)
SMEM = pl.BlockSpec(memory_space=pltpu.SMEM)
HBM = pl.BlockSpec(memory_space=pltpu.HBM)


def iota(shape, axis):
    return lax.broadcasted_iota(jnp.int32, shape, axis)


def pack_kernel(slots, src_ref, own_ref, row_ref, cnt_ref, out_ref, held):
    strips, terms, panels = src_ref.shape
    shards = out_ref.shape[0]
    own_row = own_ref[...].astype(F32)
    same = iota((strips, strips), 0) == iota((strips, strips), 1)
    earlier = iota((strips, strips), 0) < iota((strips, strips), 1)
    own_col = jnp.sum(jnp.where(same, own_row, 0.0), axis=1, keepdims=True)
    cnt_col = jnp.sum(jnp.where(same, cnt_ref[...].astype(F32), 0.0), axis=1, keepdims=True)
    ranks = jnp.sum(
        jnp.where(jnp.logical_and(own_col == own_row, earlier), 1.0, 0.0), axis=0, keepdims=True
    )
    slot_row = own_row * slots + ranks
    total = shards * slots
    placed = iota((total, strips), 0).astype(F32) == slot_row
    placing = jnp.where(placed, 1.0, 0.0).astype(BF16)
    rows = (
        jnp.sum(jnp.where(placed, row_ref[...].astype(F32) + 1.0, 0.0), axis=1, keepdims=True) - 1.0
    )
    held[...] = src_ref[...].astype(F32).reshape(strips * terms, panels)
    live = iota((strips, panels), 1).astype(F32) < cnt_col
    for first in range(0, terms, 2):
        pair = []
        for term in (first, first + 1):
            masked = jnp.where(live, held[pl.ds(term, strips, stride=terms), :], 0.0).astype(BF16)
            moved = jnp.dot(placing, masked, preferred_element_type=F32)
            pair.append(moved.reshape(shards, slots, panels))
        out_ref[:, first * slots : (first + 2) * slots, :] = jnp.concatenate(pair, axis=1).astype(
            BF16
        )
    out_ref[:, terms * slots :, :] = (
        jnp.broadcast_to(rows, (total, panels)).reshape(shards, slots, panels).astype(BF16)
    )


PAIRS = 64


def gains_kernel(blocks, first_ref, view_ref, out_ref, inward, outward, in_sem, out_sem):
    depth, taken_rows, lanes = inward.shape
    spare, own, count, observers = outward.shape
    tiles = observers // lanes
    group = taken_rows // count
    steps = view_ref.shape[0] // taken_rows
    chunk = 8 * group
    shape = (own * tiles * 8, chunk)
    to, come = iota(shape, 0), iota(shape, 1)
    block = first_ref[0] + to // (8 * tiles)
    wanted = (to % 8) * group + (to // 8 % tiles) * blocks + block
    pick = jnp.where(come == wanted, 1.0, 0.0).astype(BF16)

    def fetch(step):
        slot = lax.rem(step, depth)
        return pltpu.make_async_copy(
            view_ref.at[pl.ds(pl.multiple_of(step * taken_rows, taken_rows), taken_rows), :],
            inward.at[slot],
            in_sem.at[slot],
        )

    def leave(step):
        slot = lax.rem(step, spare)
        return pltpu.make_async_copy(
            outward.at[slot],
            out_ref.at[:, pl.ds(pl.multiple_of(step * count, count), count), :],
            out_sem.at[slot],
        )

    for step in range(depth - 1):
        fetch(step).start()

    def body(step, carry):
        @pl.when(step + depth - 1 < steps)
        def _():
            fetch(step + depth - 1).start()

        fetch(step).wait()

        @pl.when(step >= spare)
        def _():
            leave(step - spare).wait()

        slot, held = lax.rem(step, spare), lax.rem(step, depth)
        for at in range(0, count, 16):
            pair = jnp.concatenate(
                [
                    inward[held, at * group : at * group + chunk, :],
                    inward[held, at * group + chunk : at * group + 2 * chunk, :],
                ],
                axis=1,
            )
            taken = jnp.dot(pick, pair, preferred_element_type=F32)
            for turn in range(own):
                for tile in range(tiles):
                    start = (turn * tiles + tile) * 8
                    both = jnp.concatenate(
                        [taken[start : start + 8, :lanes], taken[start : start + 8, lanes:]], axis=0
                    )
                    outward[slot, turn, at : at + 16, tile * lanes : (tile + 1) * lanes] = (
                        both.astype(BF16)
                    )
        leave(step).start()
        return carry

    lax.fori_loop(0, steps, body, 0)
    for step in range(steps - spare, steps):
        leave(step).wait()


def sum_rows(slots, terms, got_refs, held, src):
    panels = src.shape[1]
    row_count = src.shape[0] // terms

    def taken(term):
        parts = [
            ref[:, term * slots : (term + 1) * slots, :].astype(F32).reshape(-1, panels)
            for ref in got_refs
        ]
        return jnp.concatenate(parts, axis=0)

    rows = taken(terms)
    hot_t = jnp.concatenate(
        [
            jnp.where(rows == (iota(rows.shape, 1) + start).astype(F32), 1.0, 0.0)
            for start in range(0, row_count, panels)
        ],
        axis=1,
    )
    hot = hot_t.T.astype(BF16)
    for term in range(terms):
        held[pl.ds(term, row_count, stride=terms), :] = jnp.dot(
            hot, taken(term).astype(BF16), preferred_element_type=F32
        )
    src[...] = held[...].astype(BF16)


def signal_kernel(slots, terms, columns, *refs):
    got_refs, refs = refs[:columns], refs[columns:]
    block_ref, bin_ref, frac_ref, gain_ref, out_ref, src, held, arr, gains, turned, sem = refs
    row_count, _, panels = bin_ref.shape
    planes, places, own, share, _ = out_ref.shape
    copies = [
        pltpu.make_async_copy(gain_ref.at[turn], gains.at[turn], sem.at[turn])
        for turn in range(own)
    ]
    for copy in copies:
        copy.start()
    sum_rows(slots, terms, got_refs, held, src)
    half = 2 * terms
    upper = iota((half, panels), 0) < terms
    place = iota((half, panels), 0).astype(F32)

    def spread(value):
        return jnp.broadcast_to(value, (half, panels))

    def weights(block, row):
        here = bin_ref[row, pl.ds(block, 1), :].astype(F32)
        past = frac_ref[row, pl.ds(block, 1), :]
        tile = jnp.floor(here * (1.0 / half))
        inner = spread(here - half * tile)
        tile = spread(tile).astype(BF16)
        low_w, high_w = spread(1.0 - past), spread(past)
        body = jnp.where(
            place == inner, low_w, jnp.where(place == inner + 1.0, high_w, 0.0)
        ).astype(BF16)
        spill = jnp.where(place + float(half - 1) == inner, high_w, 0.0).astype(BF16)
        zero = jnp.zeros((half, panels), BF16)
        tiles, before = [], None
        for index in range(NBIN // half):
            match = tile == jnp.full((half, panels), index, BF16)
            rest = zero if before is None else jnp.where(before, spill, zero)
            tiles.append(jnp.where(match, body, rest))
            before = match
        return jnp.concatenate(tiles, axis=0)

    def bin_rows(block):
        def step(index, carry):
            for inner in range(PAIRS):
                pair = index * PAIRS + inner
                where = pl.ds(pl.multiple_of(pair * half, half), half)
                rows16 = src[where, :]
                zero = jnp.zeros_like(rows16)
                lhs = jnp.concatenate(
                    [jnp.where(upper, rows16, zero), jnp.where(upper, zero, rows16)], axis=1
                )
                rhs = jnp.concatenate(
                    [weights(block, 2 * pair), weights(block, 2 * pair + 1)], axis=1
                )
                if inner % 3 < 2:
                    turned[inner] = rhs.T
                    binned = jnp.dot(lhs, turned[inner], preferred_element_type=F32)
                else:
                    binned = lax.dot_general(
                        lhs, rhs, (((1,), (1,)), ((), ())), preferred_element_type=F32
                    )
                arr[where, :] = binned.astype(BF16)
            return carry

        lax.fori_loop(0, row_count // (2 * PAIRS), step, 0)

    def block_step(turn, carry):
        bin_rows(block_ref[0] + turn)
        pltpu.make_async_copy(gain_ref.at[turn], gains.at[turn], sem.at[turn]).wait()
        out_t = lax.dot_general(
            arr[...], gains[turn], (((0,), (0,)), ((), ())), preferred_element_type=F32
        )
        out = out_t.T.astype(BF16)
        for line in range(places // columns):
            for plane in range(planes):
                for column in range(columns):
                    start = ((line * planes + plane) * columns + column) * share
                    out_ref[plane, line * columns + column, turn] = out[start : start + share, :]
        return carry

    lax.fori_loop(0, own, block_step, 0)


def on_device(sources, owners, strip_rows, panel_counts, arrival_bins, arrival_fracs, gain_table):
    strips, terms, panels = sources.shape
    shards = lax.axis_size("gx")
    columns = lax.axis_size("gy")
    cap = 2 * strips // shards
    slots = -(-cap // 8) * 8
    rows_here, blocks = arrival_bins.shape[:2]
    observers = gain_table.shape[3]
    own = blocks // columns
    devices = shards * columns
    assert rows_here <= 256 and blocks % columns == 0

    send = pl.pallas_call(
        functools.partial(pack_kernel, slots),
        out_shape=jax.ShapeDtypeStruct((shards, (terms + 1) * slots, panels), BF16),
        in_specs=[VMEM] * 4,
        out_specs=VMEM,
        scratch_shapes=[pltpu.VMEM((strips * terms, panels), F32)],
        name="pack",
    )(sources, owners.reshape(1, strips), strip_rows.reshape(1, strips), panel_counts.reshape(1, strips))

    got = lax.all_to_all(send, "gx", split_axis=0, concat_axis=0, tiled=True)
    first = lax.axis_index("gy") * own
    group = blocks * (observers // LANES)
    view = (
        gain_table.reshape(rows_here * terms, blocks, observers // LANES, LANES)
        .transpose(0, 2, 1, 3)
        .reshape(rows_here * terms * group, LANES)
    )
    own_gains = pl.pallas_call(
        functools.partial(gains_kernel, blocks),
        out_shape=jax.ShapeDtypeStruct((own, rows_here * terms, observers), BF16),
        in_specs=[SMEM, HBM],
        out_specs=HBM,
        scratch_shapes=[
            pltpu.VMEM((DEPTH, STEP * group, LANES), BF16),
            pltpu.VMEM((SPARE, own, STEP, observers), BF16),
            pltpu.SemaphoreType.DMA((DEPTH,)),
            pltpu.SemaphoreType.DMA((SPARE,)),
        ],
        name="gains",
        cost_estimate=pl.CostEstimate(
            flops=20 * gain_table.size, bytes_accessed=3 * gain_table.size, transcendentals=0
        ),
    )(first.reshape(1), view)
    got, own_gains = lax.optimization_barrier((got, own_gains))
    parts = [got]
    for turn in range(1, columns):
        parts.append(
            lax.ppermute(got, "gy", [(i, (i + turn) % columns) for i in range(columns)])
        )
    share = observers // devices
    planes, lines = shards, 1
    in_plane = [[line * planes + i for i in range(planes)] for line in range(lines)]
    in_line = [
        [(line * planes + i) * columns + j for line in range(lines) for j in range(columns)]
        for i in range(planes)
    ]
    partial = pl.pallas_call(
        functools.partial(signal_kernel, slots, terms, columns),
        out_shape=jax.ShapeDtypeStruct((planes, lines * columns, own, share, NBIN), BF16),
        in_specs=[VMEM] * columns + [SMEM] + [VMEM] * 2 + [HBM],
        out_specs=VMEM,
        scratch_shapes=[
            pltpu.VMEM((rows_here * terms, panels), BF16),
            pltpu.VMEM((rows_here * terms, panels), F32),
            pltpu.VMEM((rows_here * terms, NBIN), BF16),
            pltpu.VMEM((own, rows_here * terms, observers), BF16),
            pltpu.VMEM((PAIRS, 2 * panels, NBIN), BF16),
            pltpu.SemaphoreType.DMA((own,)),
        ],
        name="signal",
        compiler_params=pltpu.CompilerParams(vmem_limit_bytes=48 << 20),
        cost_estimate=pl.CostEstimate(
            flops=2 * own * rows_here * terms * NBIN * (observers + panels * 8),
            bytes_accessed=2 * own * rows_here * terms * observers,
            transcendentals=0,
        ),
    )(*parts, first.reshape(1), arrival_bins, arrival_fracs, own_gains)
    met = lax.all_to_all(
        partial.reshape(devices, own, share, NBIN),
        ("gx", "gy"),
        split_axis=0,
        concat_axis=0,
        tiled=True,
    )
    sums = jnp.sum(met.reshape(shards, columns, own, share, NBIN).astype(F32), axis=0)
    return jnp.transpose(sums.reshape(blocks, share, NBIN), (1, 0, 2))


def solution(mesh):
    placed = (
        P(("gx", "gy"), None, None),
        P(("gx", "gy"), None),
        P(("gx", "gy")),
        P(("gx", "gy")),
        P("gx", None, None),
        P("gx", None, None),
        P("gx", None, None, None),
    )
    return jax.shard_map(
        on_device,
        mesh=mesh,
        in_specs=placed,
        out_specs=P(("gx", "gy"), None, None),
        check_vma=False,
    )
```

```python
import functools

import jax
import jax.numpy as jnp
from jax import lax
from jax.experimental import pallas as pl
from jax.experimental.pallas import tpu as pltpu
from jax.sharding import PartitionSpec as P

NBIN = 256
LANES = 128
STEP = 128
DEPTH = 12
SPARE = 6
F32 = jnp.float32
BF16 = jnp.bfloat16
VMEM = pl.BlockSpec(memory_space=pltpu.VMEM)
SMEM = pl.BlockSpec(memory_space=pltpu.SMEM)
HBM = pl.BlockSpec(memory_space=pltpu.HBM)


def iota(shape, axis):
    return lax.broadcasted_iota(jnp.int32, shape, axis)


def pack_kernel(slots, src_ref, own_ref, row_ref, cnt_ref, out_ref, held):
    strips, terms, panels = src_ref.shape
    shards = out_ref.shape[0]
    own_row = own_ref[...].astype(F32)
    same = iota((strips, strips), 0) == iota((strips, strips), 1)
    earlier = iota((strips, strips), 0) < iota((strips, strips), 1)
    own_col = jnp.sum(jnp.where(same, own_row, 0.0), axis=1, keepdims=True)
    cnt_col = jnp.sum(jnp.where(same, cnt_ref[...].astype(F32), 0.0), axis=1, keepdims=True)
    ranks = jnp.sum(
        jnp.where(jnp.logical_and(own_col == own_row, earlier), 1.0, 0.0), axis=0, keepdims=True
    )
    slot_row = own_row * slots + ranks
    total = shards * slots
    placed = iota((total, strips), 0).astype(F32) == slot_row
    placing = jnp.where(placed, 1.0, 0.0).astype(BF16)
    rows = (
        jnp.sum(jnp.where(placed, row_ref[...].astype(F32) + 1.0, 0.0), axis=1, keepdims=True) - 1.0
    )
    held[...] = src_ref[...].astype(F32).reshape(strips * terms, panels)
    live = iota((strips, panels), 1).astype(F32) < cnt_col
    for first in range(0, terms, 2):
        pair = []
        for term in (first, first + 1):
            masked = jnp.where(live, held[pl.ds(term, strips, stride=terms), :], 0.0).astype(BF16)
            moved = jnp.dot(placing, masked, preferred_element_type=F32)
            pair.append(moved.reshape(shards, slots, panels))
        out_ref[:, first * slots : (first + 2) * slots, :] = jnp.concatenate(pair, axis=1).astype(
            BF16
        )
    out_ref[:, terms * slots :, :] = (
        jnp.broadcast_to(rows, (total, panels)).reshape(shards, slots, panels).astype(BF16)
    )


PAIRS = 128


def gains_kernel(blocks, first_ref, view_ref, out_ref, inward, outward, in_sem, out_sem):
    depth, taken_rows, lanes = inward.shape
    spare, own, count, observers = outward.shape
    tiles = observers // lanes
    group = taken_rows // count
    steps = view_ref.shape[0] // taken_rows
    chunk = 8 * group
    shape = (own * tiles * 8, chunk)
    to, come = iota(shape, 0), iota(shape, 1)
    block = first_ref[0] + to // (8 * tiles)
    wanted = (to % 8) * group + (to // 8 % tiles) * blocks + block
    pick = jnp.where(come == wanted, 1.0, 0.0).astype(BF16)

    def fetch(step):
        slot = lax.rem(step, depth)
        return pltpu.make_async_copy(
            view_ref.at[pl.ds(pl.multiple_of(step * taken_rows, taken_rows), taken_rows), :],
            inward.at[slot],
            in_sem.at[slot],
        )

    def leave(step):
        slot = lax.rem(step, spare)
        return pltpu.make_async_copy(
            outward.at[slot],
            out_ref.at[:, pl.ds(pl.multiple_of(step * count, count), count), :],
            out_sem.at[slot],
        )

    for step in range(depth - 1):
        fetch(step).start()

    def body(step, carry):
        @pl.when(step + depth - 1 < steps)
        def _():
            fetch(step + depth - 1).start()

        fetch(step).wait()

        @pl.when(step >= spare)
        def _():
            leave(step - spare).wait()

        slot, held = lax.rem(step, spare), lax.rem(step, depth)
        for at in range(0, count, 16):
            pair = jnp.concatenate(
                [
                    inward[held, at * group : at * group + chunk, :],
                    inward[held, at * group + chunk : at * group + 2 * chunk, :],
                ],
                axis=1,
            )
            taken = jnp.dot(pick, pair, preferred_element_type=F32)
            for turn in range(own):
                for tile in range(tiles):
                    start = (turn * tiles + tile) * 8
                    both = jnp.concatenate(
                        [taken[start : start + 8, :lanes], taken[start : start + 8, lanes:]], axis=0
                    )
                    outward[slot, turn, at : at + 16, tile * lanes : (tile + 1) * lanes] = (
                        both.astype(BF16)
                    )
        leave(step).start()
        return carry

    lax.fori_loop(0, steps, body, 0)
    for step in range(steps - spare, steps):
        leave(step).wait()


def sum_rows(slots, terms, got_refs, held, src):
    panels = src.shape[1]
    row_count = src.shape[0] // terms

    def taken(term):
        parts = [
            ref[:, term * slots : (term + 1) * slots, :].astype(F32).reshape(-1, panels)
            for ref in got_refs
        ]
        return jnp.concatenate(parts, axis=0)

    rows = taken(terms)
    hot_t = jnp.concatenate(
        [
            jnp.where(rows == (iota(rows.shape, 1) + start).astype(F32), 1.0, 0.0)
            for start in range(0, row_count, panels)
        ],
        axis=1,
    )
    hot = hot_t.T.astype(BF16)
    for term in range(terms):
        held[pl.ds(term, row_count, stride=terms), :] = jnp.dot(
            hot, taken(term).astype(BF16), preferred_element_type=F32
        )
    src[...] = held[...].astype(BF16)


def signal_kernel(slots, terms, columns, *refs):
    got_refs, refs = refs[:columns], refs[columns:]
    block_ref, bin_ref, frac_ref, gain_ref, out_ref, src, held, arr, gains, turned, sem = refs
    row_count, _, panels = bin_ref.shape
    planes, places, own, share, _ = out_ref.shape
    copies = [
        pltpu.make_async_copy(gain_ref.at[turn], gains.at[turn], sem.at[turn])
        for turn in range(own)
    ]
    for copy in copies:
        copy.start()
    sum_rows(slots, terms, got_refs, held, src)
    half = 2 * terms
    upper = iota((half, panels), 0) < terms
    place = iota((half, panels), 0).astype(F32)

    def spread(value):
        return jnp.broadcast_to(value, (half, panels))

    def weights(block, row):
        here = bin_ref[row, pl.ds(block, 1), :].astype(F32)
        past = frac_ref[row, pl.ds(block, 1), :]
        tile = jnp.floor(here * (1.0 / half))
        inner = spread(here - half * tile)
        tile = spread(tile).astype(BF16)
        low_w, high_w = spread(1.0 - past), spread(past)
        body = jnp.where(
            place == inner, low_w, jnp.where(place == inner + 1.0, high_w, 0.0)
        ).astype(BF16)
        spill = jnp.where(place + float(half - 1) == inner, high_w, 0.0).astype(BF16)
        zero = jnp.zeros((half, panels), BF16)
        tiles, before = [], None
        for index in range(NBIN // half):
            match = tile == jnp.full((half, panels), index, BF16)
            rest = zero if before is None else jnp.where(before, spill, zero)
            tiles.append(jnp.where(match, body, rest))
            before = match
        return jnp.concatenate(tiles, axis=0)

    def bin_rows(block):
        def step(index, carry):
            for inner in range(PAIRS):
                pair = index * PAIRS + inner
                where = pl.ds(pl.multiple_of(pair * half, half), half)
                rows16 = src[where, :]
                zero = jnp.zeros_like(rows16)
                lhs = jnp.concatenate(
                    [jnp.where(upper, rows16, zero), jnp.where(upper, zero, rows16)], axis=1
                )
                rhs = jnp.concatenate(
                    [weights(block, 2 * pair), weights(block, 2 * pair + 1)], axis=1
                )
                if inner % 3 < 2:
                    turned[inner] = rhs.T
                    binned = jnp.dot(lhs, turned[inner], preferred_element_type=F32)
                else:
                    binned = lax.dot_general(
                        lhs, rhs, (((1,), (1,)), ((), ())), preferred_element_type=F32
                    )
                arr[where, :] = binned.astype(BF16)
            return carry

        lax.fori_loop(0, row_count // (2 * PAIRS), step, 0)

    def block_step(turn, carry):
        bin_rows(block_ref[0] + turn)
        pltpu.make_async_copy(gain_ref.at[turn], gains.at[turn], sem.at[turn]).wait()
        out_t = lax.dot_general(
            arr[...], gains[turn], (((0,), (0,)), ((), ())), preferred_element_type=F32
        )
        out = out_t.T.astype(BF16)
        for line in range(places // columns):
            for plane in range(planes):
                for column in range(columns):
                    start = ((line * planes + plane) * columns + column) * share
                    out_ref[plane, line * columns + column, turn] = out[start : start + share, :]
        return carry

    lax.fori_loop(0, own, block_step, 0)


def on_device(sources, owners, strip_rows, panel_counts, arrival_bins, arrival_fracs, gain_table):
    strips, terms, panels = sources.shape
    shards = lax.axis_size("gx")
    columns = lax.axis_size("gy")
    cap = 2 * strips // shards
    slots = -(-cap // 8) * 8
    rows_here, blocks = arrival_bins.shape[:2]
    observers = gain_table.shape[3]
    own = blocks // columns
    devices = shards * columns
    assert rows_here <= 256 and blocks % columns == 0

    send = pl.pallas_call(
        functools.partial(pack_kernel, slots),
        out_shape=jax.ShapeDtypeStruct((shards, (terms + 1) * slots, panels), BF16),
        in_specs=[VMEM] * 4,
        out_specs=VMEM,
        scratch_shapes=[pltpu.VMEM((strips * terms, panels), F32)],
        name="pack",
    )(sources, owners.reshape(1, strips), strip_rows.reshape(1, strips), panel_counts.reshape(1, strips))

    got = lax.all_to_all(send, "gx", split_axis=0, concat_axis=0, tiled=True)
    first = lax.axis_index("gy") * own
    group = blocks * (observers // LANES)
    view = (
        gain_table.reshape(rows_here * terms, blocks, observers // LANES, LANES)
        .transpose(0, 2, 1, 3)
        .reshape(rows_here * terms * group, LANES)
    )
    own_gains = pl.pallas_call(
        functools.partial(gains_kernel, blocks),
        out_shape=jax.ShapeDtypeStruct((own, rows_here * terms, observers), BF16),
        in_specs=[SMEM, HBM],
        out_specs=HBM,
        scratch_shapes=[
            pltpu.VMEM((DEPTH, STEP * group, LANES), BF16),
            pltpu.VMEM((SPARE, own, STEP, observers), BF16),
            pltpu.SemaphoreType.DMA((DEPTH,)),
            pltpu.SemaphoreType.DMA((SPARE,)),
        ],
        name="gains",
        cost_estimate=pl.CostEstimate(
            flops=20 * gain_table.size, bytes_accessed=3 * gain_table.size, transcendentals=0
        ),
    )(first.reshape(1), view)
    got, own_gains = lax.optimization_barrier((got, own_gains))
    parts = [got]
    for turn in range(1, columns):
        parts.append(
            lax.ppermute(got, "gy", [(i, (i + turn) % columns) for i in range(columns)])
        )
    share = observers // devices
    planes, lines = shards, 1
    in_plane = [[line * planes + i for i in range(planes)] for line in range(lines)]
    in_line = [
        [(line * planes + i) * columns + j for line in range(lines) for j in range(columns)]
        for i in range(planes)
    ]
    partial = pl.pallas_call(
        functools.partial(signal_kernel, slots, terms, columns),
        out_shape=jax.ShapeDtypeStruct((planes, lines * columns, own, share, NBIN), BF16),
        in_specs=[VMEM] * columns + [SMEM] + [VMEM] * 2 + [HBM],
        out_specs=VMEM,
        scratch_shapes=[
            pltpu.VMEM((rows_here * terms, panels), BF16),
            pltpu.VMEM((rows_here * terms, panels), F32),
            pltpu.VMEM((rows_here * terms, NBIN), BF16),
            pltpu.VMEM((own, rows_here * terms, observers), BF16),
            pltpu.VMEM((PAIRS, 2 * panels, NBIN), BF16),
            pltpu.SemaphoreType.DMA((own,)),
        ],
        name="signal",
        compiler_params=pltpu.CompilerParams(vmem_limit_bytes=48 << 20),
        cost_estimate=pl.CostEstimate(
            flops=2 * own * rows_here * terms * NBIN * (observers + panels * 8),
            bytes_accessed=2 * own * rows_here * terms * observers,
            transcendentals=0,
        ),
    )(*parts, first.reshape(1), arrival_bins, arrival_fracs, own_gains)
    met = lax.all_to_all(
        partial.reshape(devices, own, share, NBIN),
        ("gx", "gy"),
        split_axis=0,
        concat_axis=0,
        tiled=True,
    )
    sums = jnp.sum(met.reshape(shards, columns, own, share, NBIN).astype(F32), axis=0)
    return jnp.transpose(sums.reshape(blocks, share, NBIN), (1, 0, 2))


def solution(mesh):
    placed = (
        P(("gx", "gy"), None, None),
        P(("gx", "gy"), None),
        P(("gx", "gy")),
        P(("gx", "gy")),
        P("gx", None, None),
        P("gx", None, None),
        P("gx", None, None, None),
    )
    return jax.shard_map(
        on_device,
        mesh=mesh,
        in_specs=placed,
        out_specs=P(("gx", "gy"), None, None),
        check_vma=False,
    )
```

```python
import functools

import jax
import jax.numpy as jnp
from jax import lax
from jax.experimental import pallas as pl
from jax.experimental.pallas import tpu as pltpu
from jax.sharding import PartitionSpec as P

NBIN = 256
LANES = 128
STEP = 128
DEPTH = 12
SPARE = 6
F32 = jnp.float32
BF16 = jnp.bfloat16
VMEM = pl.BlockSpec(memory_space=pltpu.VMEM)
SMEM = pl.BlockSpec(memory_space=pltpu.SMEM)
HBM = pl.BlockSpec(memory_space=pltpu.HBM)


def iota(shape, axis):
    return lax.broadcasted_iota(jnp.int32, shape, axis)


def pack_kernel(slots, src_ref, own_ref, row_ref, cnt_ref, out_ref, held):
    strips, terms, panels = src_ref.shape
    shards = out_ref.shape[0]
    own_row = own_ref[...].astype(F32)
    same = iota((strips, strips), 0) == iota((strips, strips), 1)
    earlier = iota((strips, strips), 0) < iota((strips, strips), 1)
    own_col = jnp.sum(jnp.where(same, own_row, 0.0), axis=1, keepdims=True)
    cnt_col = jnp.sum(jnp.where(same, cnt_ref[...].astype(F32), 0.0), axis=1, keepdims=True)
    ranks = jnp.sum(
        jnp.where(jnp.logical_and(own_col == own_row, earlier), 1.0, 0.0), axis=0, keepdims=True
    )
    slot_row = own_row * slots + ranks
    total = shards * slots
    placed = iota((total, strips), 0).astype(F32) == slot_row
    placing = jnp.where(placed, 1.0, 0.0).astype(BF16)
    rows = (
        jnp.sum(jnp.where(placed, row_ref[...].astype(F32) + 1.0, 0.0), axis=1, keepdims=True) - 1.0
    )
    held[...] = src_ref[...].astype(F32).reshape(strips * terms, panels)
    live = iota((strips, panels), 1).astype(F32) < cnt_col
    for first in range(0, terms, 2):
        pair = []
        for term in (first, first + 1):
            masked = jnp.where(live, held[pl.ds(term, strips, stride=terms), :], 0.0).astype(BF16)
            moved = jnp.dot(placing, masked, preferred_element_type=F32)
            pair.append(moved.reshape(shards, slots, panels))
        out_ref[:, first * slots : (first + 2) * slots, :] = jnp.concatenate(pair, axis=1).astype(
            BF16
        )
    out_ref[:, terms * slots :, :] = (
        jnp.broadcast_to(rows, (total, panels)).reshape(shards, slots, panels).astype(BF16)
    )


PAIRS = 128


def gains_kernel(blocks, first_ref, view_ref, out_ref, inward, outward, in_sem, out_sem):
    depth, taken_rows, lanes = inward.shape
    spare, own, count, observers = outward.shape
    tiles = observers // lanes
    group = taken_rows // count
    steps = view_ref.shape[0] // taken_rows
    chunk = 8 * group
    shape = (own * tiles * 8, chunk)
    to, come = iota(shape, 0), iota(shape, 1)
    block = first_ref[0] + to // (8 * tiles)
    wanted = (to % 8) * group + (to // 8 % tiles) * blocks + block
    pick = jnp.where(come == wanted, 1.0, 0.0).astype(BF16)

    def fetch(step):
        slot = lax.rem(step, depth)
        return pltpu.make_async_copy(
            view_ref.at[pl.ds(pl.multiple_of(step * taken_rows, taken_rows), taken_rows), :],
            inward.at[slot],
            in_sem.at[slot],
        )

    def leave(step):
        slot = lax.rem(step, spare)
        return pltpu.make_async_copy(
            outward.at[slot],
            out_ref.at[:, pl.ds(pl.multiple_of(step * count, count), count), :],
            out_sem.at[slot],
        )

    for step in range(depth - 1):
        fetch(step).start()

    def body(step, carry):
        @pl.when(step + depth - 1 < steps)
        def _():
            fetch(step + depth - 1).start()

        fetch(step).wait()

        @pl.when(step >= spare)
        def _():
            leave(step - spare).wait()

        slot, held = lax.rem(step, spare), lax.rem(step, depth)
        for at in range(0, count, 16):
            pair = jnp.concatenate(
                [
                    inward[held, at * group : at * group + chunk, :],
                    inward[held, at * group + chunk : at * group + 2 * chunk, :],
                ],
                axis=1,
            )
            taken = jnp.dot(pick, pair, preferred_element_type=F32)
            for turn in range(own):
                for tile in range(tiles):
                    start = (turn * tiles + tile) * 8
                    both = jnp.concatenate(
                        [taken[start : start + 8, :lanes], taken[start : start + 8, lanes:]], axis=0
                    )
                    outward[slot, turn, at : at + 16, tile * lanes : (tile + 1) * lanes] = (
                        both.astype(BF16)
                    )
        leave(step).start()
        return carry

    lax.fori_loop(0, steps, body, 0)
    for step in range(steps - spare, steps):
        leave(step).wait()


def sum_rows(slots, terms, got_refs, held, src):
    panels = src.shape[1]
    row_count = src.shape[0] // terms

    def taken(term):
        parts = [
            ref[:, term * slots : (term + 1) * slots, :].astype(F32).reshape(-1, panels)
            for ref in got_refs
        ]
        return jnp.concatenate(parts, axis=0)

    rows = taken(terms)
    hot_t = jnp.concatenate(
        [
            jnp.where(rows == (iota(rows.shape, 1) + start).astype(F32), 1.0, 0.0)
            for start in range(0, row_count, panels)
        ],
        axis=1,
    )
    hot = hot_t.T.astype(BF16)
    for term in range(terms):
        held[pl.ds(term, row_count, stride=terms), :] = jnp.dot(
            hot, taken(term).astype(BF16), preferred_element_type=F32
        )
    src[...] = held[...].astype(BF16)


def signal_kernel(slots, terms, columns, *refs):
    got_refs, refs = refs[:columns], refs[columns:]
    block_ref, bin_ref, frac_ref, gain_ref, out_ref, src, held, arr, gains, turned, sem = refs
    row_count, _, panels = bin_ref.shape
    planes, places, own, share, _ = out_ref.shape
    copies = [
        pltpu.make_async_copy(gain_ref.at[turn], gains.at[turn], sem.at[turn])
        for turn in range(own)
    ]
    for copy in copies:
        copy.start()
    sum_rows(slots, terms, got_refs, held, src)
    half = 2 * terms
    upper = iota((half, panels), 0) < terms
    place = iota((half, panels), 0).astype(F32)

    def spread(value):
        return jnp.broadcast_to(value, (half, panels))

    def weights(block, row):
        here = bin_ref[row, pl.ds(block, 1), :].astype(F32)
        past = frac_ref[row, pl.ds(block, 1), :]
        tile = jnp.floor(here * (1.0 / half))
        inner = spread(here - half * tile)
        tile = spread(tile).astype(BF16)
        low_w, high_w = spread(1.0 - past), spread(past)
        body = jnp.where(
            place == inner, low_w, jnp.where(place == inner + 1.0, high_w, 0.0)
        ).astype(BF16)
        spill = jnp.where(place + float(half - 1) == inner, high_w, 0.0).astype(BF16)
        zero = jnp.zeros((half, panels), BF16)
        tiles, before = [], None
        for index in range(NBIN // half):
            match = tile == jnp.full((half, panels), index, BF16)
            rest = zero if before is None else jnp.where(before, spill, zero)
            tiles.append(jnp.where(match, body, rest))
            before = match
        return jnp.concatenate(tiles, axis=0)

    def bin_rows(block, turn):
        def step(index, carry):
            for inner in range(PAIRS):
                pair = index * PAIRS + inner
                where = pl.ds(pl.multiple_of(pair * half, half), half)
                rows16 = src[where, :]
                zero = jnp.zeros_like(rows16)
                lhs = jnp.concatenate(
                    [jnp.where(upper, rows16, zero), jnp.where(upper, zero, rows16)], axis=1
                )
                rhs = jnp.concatenate(
                    [weights(block, 2 * pair), weights(block, 2 * pair + 1)], axis=1
                )
                if inner % 3 < 2:
                    turned[inner] = rhs.T
                    binned = jnp.dot(lhs, turned[inner], preferred_element_type=F32)
                else:
                    binned = lax.dot_general(
                        lhs, rhs, (((1,), (1,)), ((), ())), preferred_element_type=F32
                    )
                arr[turn, where, :] = binned.astype(BF16)
            return carry

        lax.fori_loop(0, row_count // (2 * PAIRS), step, 0, unroll=True)

    def block_step(turn):
        bin_rows(block_ref[0] + turn, turn)
        if turn == 0:
            for copy in copies:
                copy.wait()
        out_t = lax.dot_general(
            arr[turn], gains[turn], (((0,), (0,)), ((), ())), preferred_element_type=F32
        )
        out = out_t.T.astype(BF16)
        for line in range(places // columns):
            for plane in range(planes):
                for column in range(columns):
                    start = ((line * planes + plane) * columns + column) * share
                    out_ref[plane, line * columns + column, turn] = out[start : start + share, :]

    for turn in range(own):
        block_step(turn)


def on_device(sources, owners, strip_rows, panel_counts, arrival_bins, arrival_fracs, gain_table):
    strips, terms, panels = sources.shape
    shards = lax.axis_size("gx")
    columns = lax.axis_size("gy")
    cap = 2 * strips // shards
    slots = -(-cap // 8) * 8
    rows_here, blocks = arrival_bins.shape[:2]
    observers = gain_table.shape[3]
    own = blocks // columns
    devices = shards * columns
    assert rows_here <= 256 and blocks % columns == 0

    send = pl.pallas_call(
        functools.partial(pack_kernel, slots),
        out_shape=jax.ShapeDtypeStruct((shards, (terms + 1) * slots, panels), BF16),
        in_specs=[VMEM] * 4,
        out_specs=VMEM,
        scratch_shapes=[pltpu.VMEM((strips * terms, panels), F32)],
        name="pack",
    )(sources, owners.reshape(1, strips), strip_rows.reshape(1, strips), panel_counts.reshape(1, strips))

    got = lax.all_to_all(send, "gx", split_axis=0, concat_axis=0, tiled=True)
    first = lax.axis_index("gy") * own
    group = blocks * (observers // LANES)
    view = (
        gain_table.reshape(rows_here * terms, blocks, observers // LANES, LANES)
        .transpose(0, 2, 1, 3)
        .reshape(rows_here * terms * group, LANES)
    )
    own_gains = pl.pallas_call(
        functools.partial(gains_kernel, blocks),
        out_shape=jax.ShapeDtypeStruct((own, rows_here * terms, observers), BF16),
        in_specs=[SMEM, HBM],
        out_specs=HBM,
        scratch_shapes=[
            pltpu.VMEM((DEPTH, STEP * group, LANES), BF16),
            pltpu.VMEM((SPARE, own, STEP, observers), BF16),
            pltpu.SemaphoreType.DMA((DEPTH,)),
            pltpu.SemaphoreType.DMA((SPARE,)),
        ],
        name="gains",
        cost_estimate=pl.CostEstimate(
            flops=20 * gain_table.size, bytes_accessed=3 * gain_table.size, transcendentals=0
        ),
    )(first.reshape(1), view)
    got, own_gains = lax.optimization_barrier((got, own_gains))
    parts = [got]
    for turn in range(1, columns):
        parts.append(
            lax.ppermute(got, "gy", [(i, (i + turn) % columns) for i in range(columns)])
        )
    share = observers // devices
    planes, lines = shards, 1
    in_plane = [[line * planes + i for i in range(planes)] for line in range(lines)]
    in_line = [
        [(line * planes + i) * columns + j for line in range(lines) for j in range(columns)]
        for i in range(planes)
    ]
    partial = pl.pallas_call(
        functools.partial(signal_kernel, slots, terms, columns),
        out_shape=jax.ShapeDtypeStruct((planes, lines * columns, own, share, NBIN), BF16),
        in_specs=[VMEM] * columns + [SMEM] + [VMEM] * 2 + [HBM],
        out_specs=VMEM,
        scratch_shapes=[
            pltpu.VMEM((rows_here * terms, panels), BF16),
            pltpu.VMEM((rows_here * terms, panels), F32),
            pltpu.VMEM((own, rows_here * terms, NBIN), BF16),
            pltpu.VMEM((own, rows_here * terms, observers), BF16),
            pltpu.VMEM((PAIRS, 2 * panels, NBIN), BF16),
            pltpu.SemaphoreType.DMA((own,)),
        ],
        name="signal",
        compiler_params=pltpu.CompilerParams(vmem_limit_bytes=48 << 20),
        cost_estimate=pl.CostEstimate(
            flops=2 * own * rows_here * terms * NBIN * (observers + panels * 8),
            bytes_accessed=2 * own * rows_here * terms * observers,
            transcendentals=0,
        ),
    )(*parts, first.reshape(1), arrival_bins, arrival_fracs, own_gains)
    met = lax.all_to_all(
        partial.reshape(devices, own, share, NBIN),
        ("gx", "gy"),
        split_axis=0,
        concat_axis=0,
        tiled=True,
    )
    sums = jnp.sum(met.reshape(shards, columns, own, share, NBIN).astype(F32), axis=0)
    return jnp.transpose(sums.reshape(blocks, share, NBIN), (1, 0, 2))


def solution(mesh):
    placed = (
        P(("gx", "gy"), None, None),
        P(("gx", "gy"), None),
        P(("gx", "gy")),
        P(("gx", "gy")),
        P("gx", None, None),
        P("gx", None, None),
        P("gx", None, None, None),
    )
    return jax.shard_map(
        on_device,
        mesh=mesh,
        in_specs=placed,
        out_specs=P(("gx", "gy"), None, None),
        check_vma=False,
    )
```
